128 devices in a mesh: dp: 64 (over z_hi, x, y, core), mp: 2 (over z_lo).
Axes of the slice: x: 4, y: 4, z: 4 (z_hi: 2, z_lo: 2; z = z_hi * 2 + z_lo), core: 2. Of those that a mesh axis runs over, the one named last changes fastest.
Arguments:
- inputs: bfloat16 [8192, 1792], P('dp', 'mp'), may hold values from -6 to 6
- cotangent: bfloat16 [8192, 1792], P('dp', 'mp'), may hold values from -6 to 6
- gate_weight: bfloat16 [9472, 1792], P(('mp', 'dp')), may hold values from -0.125 to 0.125
- up_weight: bfloat16 [9472, 1792], P(('mp', 'dp')), may hold values from -0.125 to 0.125
- down_weight: bfloat16 [9472, 1792], P(('mp', 'dp')), may hold values from -0.0625 to 0.0625
Outputs:
- input_grad: bfloat16 [8192, 1792], P('dp', 'mp')
- gate_grad: bfloat16 [9472, 1792], P(('mp', 'dp'))
The draws below stay inside these ranges and needn't reach their ends.
All inputs are finite; a program needn't handle non-finite values.
Results may differ from the reference program's by a relative error of at most 0.009.
Values may be sent and summed in bfloat16 or wider, within the bound.
No kernel may reach another device: no remote copies, remote signals or barrier semaphores. Data moves between devices by JAX's collectives and lax.ppermute only.
A program may use at most 320 MiB of HBM per device.

```python
import jax
import jax.numpy as jnp
from jax import lax

D = 1792
FF = 9472
TOKENS = 8192


def levels(stream_key, shape, cuts, least, high):
    def one(dim, blocks):
        steps = jax.random.uniform(jax.random.fold_in(jax.random.fold_in(stream_key, 6), dim), (blocks,), jnp.float32, least / len(cuts), high / len(cuts))
        return jnp.repeat(jnp.exp(steps), shape[dim] // blocks).reshape((-1,) + (1,) * (len(shape) - dim - 1))

    level = one(*cuts[0])
    for cut in cuts[1:]:
        level = level * one(*cut)
    return level


def centred(own_key, extent, spread, limit, shards=(), held_as=jnp.bfloat16):
    values = jax.random.normal(own_key, extent, jnp.float32) * spread
    if len(shards) > 0:
        values = levels(own_key, extent, shards, -0.22, 0.18) * values
    return jnp.clip(values, min=-limit, max=limit).astype(held_as)


def setup_inputs(seed: int = 0) -> dict:
    streams_of = jax.random.split(jax.random.key(seed), 6)
    return {
        "inputs": centred(streams_of[0], (TOKENS, D), 1.0, 6.0, ((0, 64), (1, 2))),
        "cotangent": centred(streams_of[1], (TOKENS, D), 1.0, 6.0, ((0, 64), (1, 2))),
        "gate_weight": centred(streams_of[2], (FF, D), D ** -0.5, 0.125, ((0, 128),)),
        "up_weight": centred(streams_of[3], (FF, D), D ** -0.5, 0.125, ((0, 128),)),
        "down_weight": centred(streams_of[4], (FF, D), FF ** -0.5, 0.0625, ((0, 128),)),
    }


def tdot(left, right):
    return lax.dot_general(left, right, (((0,), (0,)), ((), ())), preferred_element_type=jnp.float32)


def rdot(left, right):
    return lax.dot_general(left, right, (((1,), (1,)), ((), ())), preferred_element_type=jnp.float32)


def reference(inputs, cotangent, gate_weight, up_weight, down_weight):
    gate = rdot(inputs, gate_weight)
    up = rdot(inputs, up_weight)
    sig = jax.nn.sigmoid(gate)
    act = gate * sig
    dhidden = rdot(cotangent, down_weight)
    dup = (dhidden * act).astype(jnp.bfloat16)
    dgate = (dhidden * up * sig * (1.0 + gate * (1.0 - sig))).astype(jnp.bfloat16)
    gate_grad = tdot(dgate, inputs).astype(jnp.bfloat16)
    input_grad = jnp.dot(dgate, gate_weight, preferred_element_type=jnp.float32)
    input_grad = input_grad + jnp.dot(dup, up_weight, preferred_element_type=jnp.float32)
    return input_grad.astype(jnp.bfloat16), gate_grad
```

```python
import jax
import jax.numpy as jnp
from jax import lax
from jax.sharding import Mesh
from jax.sharding import PartitionSpec as P

DP = ("dp_0", "dp_1", "dp_2", "dp_3")
MP_DP = ("mp", "dp_0", "dp_1", "dp_2", "dp_3")
X, Y, CORE = "dp_1", "dp_2", "dp_3"


F32, BF16 = jnp.float32, jnp.bfloat16
ROWS = 80


def shift(x, axis, by):
    n = lax.axis_size(axis)
    return lax.ppermute(x, axis, [(i, (i - by) % n) for i in range(n)])


def swap_p(x):
    return lax.ppermute(x, "mp", [(0, 1), (1, 0)])


def swap_q(x):
    return lax.ppermute(x, ("dp_0", "mp"), [(0, 3), (3, 0), (1, 2), (2, 1)])


def swap_pq(x):
    return lax.ppermute(x, "dp_0", [(0, 1), (1, 0)])


def ring_gather(x, fwd, bwd, dim, cut):
    a, b = fwd(x), bwd(x)
    n = x.shape[dim]
    far = (
        fwd(lax.slice_in_dim(a, 0, cut, axis=dim)),
        bwd(lax.slice_in_dim(b, cut, n, axis=dim)),
    )
    return x, a, b, jnp.concatenate(far, axis=dim)


def rdot(left, right):
    return lax.dot_general(left, right, (((1,), (1,)), ((), ())), preferred_element_type=F32)


def total(*parts):
    out = parts[0].astype(F32)
    for p in parts[1:]:
        out = out + p.astype(F32)
    return out.astype(BF16)


def yfwd(x):
    return shift(x, Y, 1)


def ybwd(x):
    return shift(x, Y, -1)


def xfwd(x):
    return shift(x, X, 1)


def xbwd(x):
    return shift(x, X, -1)


def core_swap(x):
    return shift(x, CORE, 1)


def zq_gather(x, dim, cut):
    a, b = swap_p(x), swap_q(x)
    n = x.shape[dim]
    far = (
        swap_q(lax.slice_in_dim(a, 0, cut, axis=dim)),
        swap_p(lax.slice_in_dim(b, cut, n, axis=dim)),
    )
    return x, a, b, jnp.concatenate(far, axis=dim)


def per_device(inputs, cotangent, gate_weight, up_weight, down_weight):
    half = inputs.shape[1]
    t = inputs.shape[0]
    side = lax.axis_index("mp")
    pad = ((0, ROWS - gate_weight.shape[0]), (0, 0))

    def own_first(w):
        w = jnp.pad(w, pad)
        return jnp.where(side == 0, w, jnp.concatenate([w[:, half:], w[:, :half]], axis=1))

    own_w = jnp.concatenate([own_first(w) for w in (gate_weight, up_weight, down_weight)], axis=0)
    along_x = ring_gather(own_w, xfwd, xbwd, 0, 128)
    pieces = []
    for w in along_x:
        pieces += [w, core_swap(w)]
    wg = jnp.concatenate([w[:ROWS] for w in pieces], axis=0)
    wu = jnp.concatenate([w[ROWS : 2 * ROWS] for w in pieces], axis=0)
    wd = jnp.concatenate([w[2 * ROWS :] for w in pieces], axis=0)

    in_y = jnp.stack(ring_gather(inputs, yfwd, ybwd, 0, t // 2))
    i0, ip, iq, ipq = zq_gather(in_y, 0, 2)
    x = jnp.concatenate(
        [
            jnp.concatenate([i0.reshape(-1, half), ip.reshape(-1, half)], axis=1),
            jnp.concatenate([ipq.reshape(-1, half), iq.reshape(-1, half)], axis=1),
        ],
        axis=0,
    )
    c_z = jnp.stack(zq_gather(cotangent, 0, t // 2))
    c = jnp.stack(ring_gather(c_z, yfwd, ybwd, 0, 2))
    c = jnp.concatenate(
        [
            jnp.concatenate([c[:, 0].reshape(-1, half), c[:, 1].reshape(-1, half)], axis=1),
            jnp.concatenate([c[:, 3].reshape(-1, half), c[:, 2].reshape(-1, half)], axis=1),
        ],
        axis=0,
    )

    gate = rdot(wg, x)
    up = rdot(wu, x)
    dhidden = rdot(wd, c)
    sig = jax.nn.sigmoid(gate)
    act = gate * sig
    dup = (dhidden * act).astype(BF16)
    dgate = (dhidden * up * sig * (1.0 + gate * (1.0 - sig))).astype(BF16)

    gi = lax.dot_general(
        jnp.concatenate([dgate, dup], axis=0),
        jnp.concatenate([wg, wu], axis=0),
        (((0,), (0,)), ((), ())),
        preferred_element_type=F32,
    ).astype(BF16)
    gi = gi.reshape(2, 4, 2, t // 2, 2, half)
    a = gi[:, :, 0]
    za = total(a[0, :, :, 0], swap_p(a[0, :, :, 1]), swap_pq(a[1, :, :, 0]), swap_q(a[1, :, :, 1]))
    ya = total(za[0], shift(za[1], Y, -1), shift(za[2], Y, 1), shift(za[3], Y, 2))
    b = gi[:, :, 1]
    yb = total(b[:, 0], shift(b[:, 1], Y, -1), shift(b[:, 2], Y, 1), shift(b[:, 3], Y, 2))
    zb = total(yb[0, :, 0], swap_p(yb[0, :, 1]), swap_pq(yb[1, :, 0]), swap_q(yb[1, :, 1]))
    input_grad = jnp.concatenate([ya, zb], axis=0)

    gg = jnp.dot(dgate, x, preferred_element_type=F32).astype(BF16)
    gg = gg.reshape(4, 2, ROWS, 2 * half)
    cg = total(gg[:, 0], core_swap(gg[:, 1]))
    gw = total(cg[0], shift(cg[1], X, -1), shift(cg[2], X, 1), shift(cg[3], X, 2))
    gw = gw[: gate_weight.shape[0]]
    gate_grad = jnp.where(side == 0, gw, jnp.concatenate([gw[:, half:], gw[:, :half]], axis=1))
    return input_grad, gate_grad


def solution(mesh):
    torus = Mesh(
        mesh.devices.reshape(2, 4, 4, 2, mesh.shape["mp"]), ("dp_0", "dp_1", "dp_2", "dp_3", "mp")
    )
    return jax.shard_map(
        per_device,
        mesh=torus,
        in_specs=(P(DP, "mp"), P(DP, "mp"), P(MP_DP, None), P(MP_DP, None), P(MP_DP, None)),
        out_specs=(P(DP, "mp"), P(MP_DP, None)),
        check_vma=False,
    )
```

```python
import itertools

import jax
import jax.numpy as jnp
from jax import lax
from jax.experimental import pallas as pl
from jax.experimental.pallas import tpu as pltpu
from jax.sharding import Mesh
from jax.sharding import PartitionSpec as P

DP = ("dp_0", "dp_1", "dp_2", "dp_3")
MP_DP = ("mp", "dp_0", "dp_1", "dp_2", "dp_3")
X, CORE = "dp_1", "dp_3"
PLANE = ("dp_0", "dp_2", "dp_3", "mp")
SIZES = (2, 4, 2, 2)


F32, BF16 = jnp.float32, jnp.bfloat16
ROWS = 80
VMEM = pl.BlockSpec(memory_space=pltpu.VMEM)
SMEM = pl.BlockSpec(memory_space=pltpu.SMEM)

MOVES = {
    "y+": lambda z, y: (z, (y + 1) % 4),
    "y-": lambda z, y: (z, (y - 1) % 4),
    "y2": lambda z, y: (z, (y + 2) % 4),
    "P": lambda z, y: (z ^ 1, y),
    "Q": lambda z, y: (3 - z, y),
    "PQ": lambda z, y: (z ^ 2, y),
}


def fetch(x, on_core_0, on_core_1, cross=False):
    pairs = []

    def index(zh, y, core, zl):
        return ((zh * SIZES[1] + y) * SIZES[2] + core) * SIZES[3] + zl

    for zh, y, core, zl in itertools.product(*(range(n) for n in SIZES)):
        sender = 1 - core if cross else core
        z_from, y_from = MOVES[on_core_1 if sender else on_core_0](zh * 2 + zl, y)
        pairs.append((index(z_from // 2, y_from, sender, z_from % 2), index(zh, y, core, zl)))
    return lax.ppermute(x, PLANE, pairs)


def shift(x, axis, by):
    n = lax.axis_size(axis)
    return lax.ppermute(x, axis, [(i, (i - by) % n) for i in range(n)])


def rdot(left, right):
    return lax.dot_general(left, right, (((1,), (1,)), ((), ())), preferred_element_type=F32)


def total(*parts):
    out = parts[0].astype(F32)
    for p in parts[1:]:
        out = out + p.astype(F32)
    return out.astype(BF16)


def prepare_body(side_ref, g_ref, u_ref, d_ref, out_ref):
    n, full = g_ref.shape
    half = full // 2
    side = side_ref[0]
    out_ref[...] = jnp.zeros_like(out_ref)
    for s in range(2):

        @pl.when(side == s)
        def _():
            for k, ref in enumerate((g_ref, u_ref, d_ref)):
                for f in range(2):
                    src = (f + s) % 2
                    out_ref[k * ROWS : k * ROWS + n, f * half : (f + 1) * half] = ref[
                        :, src * half : (src + 1) * half
                    ]


def prepare(side, gate_weight, up_weight, down_weight):
    full = gate_weight.shape[1]
    return pl.pallas_call(
        prepare_body,
        out_shape=jax.ShapeDtypeStruct((3 * ROWS, full), BF16),
        in_specs=[SMEM, VMEM, VMEM, VMEM],
        out_specs=VMEM,
        compiler_params=pltpu.CompilerParams(vmem_limit_bytes=8 * 1024 * 1024),
        cost_estimate=pl.CostEstimate(flops=2_000_000, bytes_accessed=1_700_000, transcendentals=0),
        name="prepare",
    )(side.reshape(1), gate_weight, up_weight, down_weight)


def assemble_body(core_ref, m0, m1, m2, m3, r0, r1, r2, r3, x0_ref, x1_ref, c0_ref, c1_ref):
    mine, received = (m0, m1, m2, m3), (r0, r1, r2, r3)
    half = m0.shape[1]
    t = m3.shape[0] // 4
    core = core_ref[0]
    position = {(0, 0): 0, (0, 1): 1, (1, 0): 3, (1, 1): 2}

    for k in range(2):

        @pl.when(core == k)
        def _():
            inputs, cotangent = (mine, received) if k == 0 else (received, mine)
            for g, y, f in itertools.product(range(2), range(4), range(2)):
                block = g * 4 + y if k == 0 else y * 2 + g
                z = position[g, f]
                x_ref, c_ref = ((x0_ref, c0_ref), (x1_ref, c1_ref))[block // 4]
                block = block % 4
                rows, cols = slice(block * t, (block + 1) * t), slice(f * half, (f + 1) * half)
                x_ref[rows, cols] = inputs[z][y * t : (y + 1) * t]
                c_ref[rows, cols] = cotangent[y][z * t : (z + 1) * t]


def assemble(core, mine, received):
    rows, half = mine[3].shape
    shape = jax.ShapeDtypeStruct((rows, 2 * half), BF16)
    return pl.pallas_call(
        assemble_body,
        out_shape=(shape,) * 4,
        in_specs=[SMEM] + [VMEM] * 8,
        out_specs=(VMEM,) * 4,
        compiler_params=pltpu.CompilerParams(vmem_limit_bytes=30 * 1024 * 1024),
        cost_estimate=pl.CostEstimate(flops=4_000_000, bytes_accessed=15_000_000, transcendentals=0),
        name="assemble",
    )(core.reshape(1), *mine, *received)


def per_device(inputs, cotangent, gate_weight, up_weight, down_weight):
    t, half = inputs.shape
    side, core = lax.axis_index("mp"), lax.axis_index(CORE)
    cat = jnp.concatenate
    hold = lax.optimization_barrier

    keep = jnp.where(core == 0, inputs, cotangent)
    give = jnp.where(core == 0, cotangent, inputs)
    first = cat([keep, shift(give, CORE, 1)])
    ring = [first, fetch(first, "y+", "P"), fetch(first, "y-", "Q"), fetch(first, "y2", "PQ")]
    g = hold(cat([v[:t] for v in ring] + [v[t:] for v in ring]))
    a, b = fetch(g, "P", "y+"), fetch(g, "Q", "y-")
    n = 4 * t
    far = fetch(a[:n], "Q", "y+")
    far_received = fetch(b[n:], "P", "y-", cross=True)
    mine = (g, a, b, far)
    received = (shift(g[n:], CORE, 1), shift(a[n:], CORE, 1), shift(b[n:], CORE, 1), far_received)

    own_w = prepare(side, gate_weight, up_weight, down_weight)
    wf, wb = shift(own_w, X, 1), shift(own_w, X, -1)
    wff = cat([shift(wf[:128], X, 1), shift(wb[128:], X, -1)])
    pieces = []
    for w in (own_w, wf, wb, wff):
        pieces += [w, shift(w, CORE, 1)]
    wgu = hold(cat([w[:ROWS] for w in pieces] + [w[ROWS : 2 * ROWS] for w in pieces]))
    wd = hold(cat([w[2 * ROWS :] for w in pieces]))
    ff = wd.shape[0]

    x0, x1, c0, c1 = assemble(core, mine, received)

    def hidden_grads(x, c):
        gate = rdot(wgu[:ff], x)
        up = rdot(wgu[ff:], x)
        dhidden = rdot(wd, c)
        sig = jax.nn.sigmoid(gate)
        act = gate * sig
        dup = (dhidden * act).astype(BF16)
        dgate = (dhidden * up * sig * (1.0 + gate * (1.0 - sig))).astype(BF16)
        return hold((dgate, dup))

    def input_partials(dgate, dup, order):
        gi = hold(
            lax.dot_general(
                cat([dgate, dup]), wgu, (((0,), (0,)), ((), ())), preferred_element_type=F32
            ).astype(BF16)
        )
        on_0 = (gi[:, :half], gi[:, half:])
        on_1 = []
        for k in order:
            v = gi[2 * k * t : 2 * (k + 1) * t]
            on_1.append(cat([v[:t, :half], v[:t, half:], v[t:, half:], v[t:, :half]]))
        return hold(tuple(jnp.where(core == 0, u, v) for u, v in zip(on_0, on_1)))

    dg1, du1 = hidden_grads(x1, c1)
    far_part, back_part = input_partials(dg1, du1, (1, 0))
    got_far = fetch(far_part, "PQ", "y2")
    got_back = fetch(back_part, "Q", "y+")
    x0, c0, far_part, back_part = hold((x0, c0, far_part, back_part))
    dg0, du0 = hidden_grads(x0, c0)
    own_part, fwd_part = input_partials(dg0, du0, (0, 1))
    got_fwd = fetch(fwd_part, "P", "y-")

    gg = hold(
        (
            jnp.dot(dg0, x0, preferred_element_type=F32)
            + jnp.dot(dg1, x1, preferred_element_type=F32)
        ).astype(BF16)
    )
    r = ROWS
    own = cat([gg[2 * k * r : (2 * k + 1) * r] for k in range(4)])
    theirs = cat([gg[(2 * k + 1) * r : (2 * k + 2) * r] for k in range(4)])
    theirs = shift(theirs, CORE, 1)
    cg = hold(total(own, theirs))
    gw = total(
        cg[:r],
        shift(cg[r : 2 * r], X, -1),
        shift(cg[2 * r : 3 * r], X, 1),
        shift(cg[3 * r :], X, 2),
    )

    s = total(own_part, got_fwd, got_back, got_far)
    s = hold(tuple(s[k * t : (k + 1) * t] for k in range(4)))
    input_grad = total(
        s[0], fetch(s[1], "y-", "P"), fetch(s[2], "y+", "Q"), fetch(s[3], "y2", "PQ")
    )

    gw = gw[: gate_weight.shape[0]]
    gate_grad = jnp.where(side == 0, gw, cat([gw[:, half:], gw[:, :half]], axis=1))
    return input_grad, gate_grad


def solution(mesh):
    torus = Mesh(
        mesh.devices.reshape(2, 4, 4, 2, mesh.shape["mp"]), ("dp_0", "dp_1", "dp_2", "dp_3", "mp")
    )

    return jax.shard_map(
        per_device,
        mesh=torus,
        in_specs=(P(DP, "mp"), P(DP, "mp"), P(MP_DP, None), P(MP_DP, None), P(MP_DP, None)),
        out_specs=(P(DP, "mp"), P(MP_DP, None)),
        check_vma=False,
    )
```

```python
import itertools

import jax
import jax.numpy as jnp
from jax import lax
from jax.experimental import pallas as pl
from jax.experimental.pallas import tpu as pltpu
from jax.sharding import Mesh
from jax.sharding import PartitionSpec as P

DP = ("dp_0", "dp_1", "dp_2", "dp_3")
MP_DP = ("mp", "dp_0", "dp_1", "dp_2", "dp_3")
X, CORE = "dp_1", "dp_3"
PLANE = ("dp_0", "dp_2", "dp_3", "mp")
SIZES = (2, 4, 2, 2)


F32, BF16 = jnp.float32, jnp.bfloat16
ROWS = 80
VMEM = pl.BlockSpec(memory_space=pltpu.VMEM)
SMEM = pl.BlockSpec(memory_space=pltpu.SMEM)

MOVES = {
    "y+": lambda z, y: (z, (y + 1) % 4),
    "y-": lambda z, y: (z, (y - 1) % 4),
    "y2": lambda z, y: (z, (y + 2) % 4),
    "P": lambda z, y: (z ^ 1, y),
    "Q": lambda z, y: (3 - z, y),
    "PQ": lambda z, y: (z ^ 2, y),
}


def fetch(x, on_core_0, on_core_1, cross=False):
    pairs = []

    def index(zh, y, core, zl):
        return ((zh * SIZES[1] + y) * SIZES[2] + core) * SIZES[3] + zl

    for zh, y, core, zl in itertools.product(*(range(n) for n in SIZES)):
        sender = 1 - core if cross else core
        z_from, y_from = MOVES[on_core_1 if sender else on_core_0](zh * 2 + zl, y)
        pairs.append((index(z_from // 2, y_from, sender, z_from % 2), index(zh, y, core, zl)))
    return lax.ppermute(x, PLANE, pairs)


def shift(x, axis, by):
    n = lax.axis_size(axis)
    return lax.ppermute(x, axis, [(i, (i - by) % n) for i in range(n)])


def rdot(left, right):
    return lax.dot_general(left, right, (((1,), (1,)), ((), ())), preferred_element_type=F32)


def total(*parts):
    out = parts[0].astype(F32)
    for p in parts[1:]:
        out = out + p.astype(F32)
    return out.astype(BF16)


def prepare_body(side_ref, g_ref, u_ref, d_ref, out_ref):
    n, full = g_ref.shape
    half = full // 2
    side = side_ref[0]
    out_ref[...] = jnp.zeros_like(out_ref)
    for s in range(2):

        @pl.when(side == s)
        def _():
            for k, ref in enumerate((g_ref, u_ref, d_ref)):
                for f in range(2):
                    src = (f + s) % 2
                    out_ref[k * ROWS : k * ROWS + n, f * half : (f + 1) * half] = ref[
                        :, src * half : (src + 1) * half
                    ]


def prepare(side, gate_weight, up_weight, down_weight):
    full = gate_weight.shape[1]
    return pl.pallas_call(
        prepare_body,
        out_shape=jax.ShapeDtypeStruct((3 * ROWS, full), BF16),
        in_specs=[SMEM, VMEM, VMEM, VMEM],
        out_specs=VMEM,
        compiler_params=pltpu.CompilerParams(vmem_limit_bytes=8 * 1024 * 1024),
        cost_estimate=pl.CostEstimate(flops=2_000_000, bytes_accessed=1_700_000, transcendentals=0),
        name="prepare",
    )(side.reshape(1), gate_weight, up_weight, down_weight)


def assemble_body(core_ref, m0, m1, m2, m3, r0, r1, r2, r3, x0_ref, x1_ref, c0_ref, c1_ref):
    mine, received = (m0, m1, m2, m3), (r0, r1, r2, r3)
    half = m0.shape[1]
    t = m3.shape[0] // 4
    core = core_ref[0]
    position = {(0, 0): 0, (0, 1): 1, (1, 0): 3, (1, 1): 2}

    for k in range(2):

        @pl.when(core == k)
        def _():
            inputs, cotangent = (mine, received) if k == 0 else (received, mine)
            for g, y, f in itertools.product(range(2), range(4), range(2)):
                block = g * 4 + y if k == 0 else y * 2 + g
                z = position[g, f]
                x_ref, c_ref = ((x0_ref, c0_ref), (x1_ref, c1_ref))[block // 4]
                block = block % 4
                rows, cols = slice(block * t, (block + 1) * t), slice(f * half, (f + 1) * half)
                x_ref[rows, cols] = inputs[z][y * t : (y + 1) * t]
                c_ref[rows, cols] = cotangent[y][z * t : (z + 1) * t]


def assemble(core, mine, received):
    rows, half = mine[3].shape
    shape = jax.ShapeDtypeStruct((rows, 2 * half), BF16)
    return pl.pallas_call(
        assemble_body,
        out_shape=(shape,) * 4,
        in_specs=[SMEM] + [VMEM] * 8,
        out_specs=(VMEM,) * 4,
        compiler_params=pltpu.CompilerParams(vmem_limit_bytes=30 * 1024 * 1024),
        cost_estimate=pl.CostEstimate(flops=4_000_000, bytes_accessed=15_000_000, transcendentals=0),
        name="assemble",
    )(core.reshape(1), *mine, *received)


def per_device(inputs, cotangent, gate_weight, up_weight, down_weight):
    t, half = inputs.shape
    side, core = lax.axis_index("mp"), lax.axis_index(CORE)
    cat = jnp.concatenate
    hold = lax.optimization_barrier

    keep = jnp.where(core == 0, inputs, cotangent)
    give = jnp.where(core == 0, cotangent, inputs)
    first = cat([keep, shift(give, CORE, 1)])
    f, b = fetch(first, "y+", "P"), fetch(first, "y-", "Q")
    far = fetch(first, "y2", "PQ")
    g_own = hold(cat([v[:t] for v in (first, f, b, far)]))
    g_other = hold(cat([v[t:] for v in (first, f, b, far)]))
    a_own = fetch(g_own, "P", "y+")
    b_other = fetch(g_other, "Q", "y-")
    a_other = fetch(g_other, "P", "y+")
    b_own = fetch(g_own, "Q", "y-")
    mine = (g_own, a_own, b_own, fetch(a_own, "Q", "y+"))
    received = (
        shift(g_other, CORE, 1),
        shift(a_other, CORE, 1),
        shift(b_other, CORE, 1),
        fetch(b_other, "P", "y-", cross=True),
    )

    own_w = prepare(side, gate_weight, up_weight, down_weight)
    wf, wb = shift(own_w, X, 1), shift(own_w, X, -1)
    wff = cat([shift(wf[:128], X, 1), shift(wb[128:], X, -1)])
    pieces = []
    for w in (own_w, wf, wb, wff):
        pieces += [w, shift(w, CORE, 1)]
    wgu = hold(cat([w[:ROWS] for w in pieces] + [w[ROWS : 2 * ROWS] for w in pieces]))
    wd = hold(cat([w[2 * ROWS :] for w in pieces]))
    ff = wd.shape[0]

    x0, x1, c0, c1 = assemble(core, mine, received)

    def hidden_grads(x, c):
        gate = rdot(wgu[:ff], x)
        up = rdot(wgu[ff:], x)
        dhidden = rdot(wd, c)
        sig = jax.nn.sigmoid(gate)
        act = gate * sig
        dup = (dhidden * act).astype(BF16)
        dgate = (dhidden * up * sig * (1.0 + gate * (1.0 - sig))).astype(BF16)
        return hold((dgate, dup))

    def input_partials(dgate, dup, order):
        gi = hold(
            lax.dot_general(
                cat([dgate, dup]), wgu, (((0,), (0,)), ((), ())), preferred_element_type=F32
            ).astype(BF16)
        )
        on_0 = (gi[:, :half], gi[:, half:])
        on_1 = []
        for k in order:
            v = gi[2 * k * t : 2 * (k + 1) * t]
            on_1.append(cat([v[:t, :half], v[:t, half:], v[t:, half:], v[t:, :half]]))
        return hold(tuple(jnp.where(core == 0, u, v) for u, v in zip(on_0, on_1)))

    dg1, du1 = hidden_grads(x1, c1)
    far_part, back_part = input_partials(dg1, du1, (1, 0))
    got_far = fetch(far_part, "PQ", "y2")
    got_back = fetch(back_part, "Q", "y+")
    x0, c0, far_part, back_part = hold((x0, c0, far_part, back_part))
    dg0, du0 = hidden_grads(x0, c0)
    own_part, fwd_part = input_partials(dg0, du0, (0, 1))
    got_fwd = fetch(fwd_part, "P", "y-")
    dg0, dg1, own_part, fwd_part = hold((dg0, dg1, own_part, fwd_part))

    gg = hold(
        (
            jnp.dot(dg0, x0, preferred_element_type=F32)
            + jnp.dot(dg1, x1, preferred_element_type=F32)
        ).astype(BF16)
    )
    r = ROWS
    own = cat([gg[2 * k * r : (2 * k + 1) * r] for k in range(4)])
    theirs = cat([gg[(2 * k + 1) * r : (2 * k + 2) * r] for k in range(4)])
    theirs = shift(theirs, CORE, 1)
    cg = hold(total(own, theirs))
    gw = total(
        cg[:r],
        shift(cg[r : 2 * r], X, -1),
        shift(cg[2 * r : 3 * r], X, 1),
        shift(cg[3 * r :], X, 2),
    )

    s = total(own_part, got_fwd, got_back, got_far)
    s = hold(tuple(s[k * t : (k + 1) * t] for k in range(4)))
    input_grad = total(
        s[0], fetch(s[1], "y-", "P"), fetch(s[2], "y+", "Q"), fetch(s[3], "y2", "PQ")
    )

    gw = gw[: gate_weight.shape[0]]
    gate_grad = jnp.where(side == 0, gw, cat([gw[:, half:], gw[:, :half]], axis=1))
    return input_grad, gate_grad


def solution(mesh):
    torus = Mesh(
        mesh.devices.reshape(2, 4, 4, 2, mesh.shape["mp"]), ("dp_0", "dp_1", "dp_2", "dp_3", "mp")
    )

    return jax.shard_map(
        per_device,
        mesh=torus,
        in_specs=(P(DP, "mp"), P(DP, "mp"), P(MP_DP, None), P(MP_DP, None), P(MP_DP, None)),
        out_specs=(P(DP, "mp"), P(MP_DP, None)),
        check_vma=False,
    )
```

```python
import itertools

import jax
import jax.numpy as jnp
from jax import lax
from jax.experimental import pallas as pl
from jax.experimental.pallas import tpu as pltpu
from jax.sharding import Mesh
from jax.sharding import PartitionSpec as P

DP = ("dp_0", "dp_1", "dp_2", "dp_3")
MP_DP = ("mp", "dp_0", "dp_1", "dp_2", "dp_3")
X, CORE = "dp_1", "dp_3"
PLANE = ("dp_0", "dp_2", "dp_3", "mp")
SIZES = (2, 4, 2, 2)


F32, BF16 = jnp.float32, jnp.bfloat16
ROWS = 80
VMEM = pl.BlockSpec(memory_space=pltpu.VMEM)
SMEM = pl.BlockSpec(memory_space=pltpu.SMEM)

MOVES = {
    "y+": lambda z, y: (z, (y + 1) % 4),
    "y-": lambda z, y: (z, (y - 1) % 4),
    "y2": lambda z, y: (z, (y + 2) % 4),
    "P": lambda z, y: (z ^ 1, y),
    "Q": lambda z, y: (3 - z, y),
    "PQ": lambda z, y: (z ^ 2, y),
}


def fetch(x, on_core_0, on_core_1, cross=False):
    pairs = []

    def index(zh, y, core, zl):
        return ((zh * SIZES[1] + y) * SIZES[2] + core) * SIZES[3] + zl

    for zh, y, core, zl in itertools.product(*(range(n) for n in SIZES)):
        sender = 1 - core if cross else core
        z_from, y_from = MOVES[on_core_1 if sender else on_core_0](zh * 2 + zl, y)
        pairs.append((index(z_from // 2, y_from, sender, z_from % 2), index(zh, y, core, zl)))
    return lax.ppermute(x, PLANE, pairs)


def shift(x, axis, by):
    n = lax.axis_size(axis)
    return lax.ppermute(x, axis, [(i, (i - by) % n) for i in range(n)])


def rdot(left, right):
    return lax.dot_general(left, right, (((1,), (1,)), ((), ())), preferred_element_type=F32)


def total(*parts):
    out = parts[0].astype(F32)
    for p in parts[1:]:
        out = out + p.astype(F32)
    return out.astype(BF16)


def prepare_body(side_ref, g_ref, u_ref, d_ref, out_ref):
    n, full = g_ref.shape
    half = full // 2
    side = side_ref[0]
    out_ref[...] = jnp.zeros_like(out_ref)
    for s in range(2):

        @pl.when(side == s)
        def _():
            for k, ref in enumerate((g_ref, u_ref, d_ref)):
                for f in range(2):
                    src = (f + s) % 2
                    out_ref[k * ROWS : k * ROWS + n, f * half : (f + 1) * half] = ref[
                        :, src * half : (src + 1) * half
                    ]


def prepare(side, gate_weight, up_weight, down_weight):
    full = gate_weight.shape[1]
    return pl.pallas_call(
        prepare_body,
        out_shape=jax.ShapeDtypeStruct((3 * ROWS, full), BF16),
        in_specs=[SMEM, VMEM, VMEM, VMEM],
        out_specs=VMEM,
        compiler_params=pltpu.CompilerParams(vmem_limit_bytes=8 * 1024 * 1024),
        cost_estimate=pl.CostEstimate(flops=2_000_000, bytes_accessed=1_700_000, transcendentals=0),
        name="prepare",
    )(side.reshape(1), gate_weight, up_weight, down_weight)


def assemble_body(core_ref, m0, m1, m2, m3, r0, r1, r2, r3, x_ref, c_ref):
    mine, received = (m0, m1, m2, m3), (r0, r1, r2, r3)
    half = m0.shape[1]
    t = m3.shape[0] // 4
    core = core_ref[0]
    position = {(0, 0): 0, (0, 1): 1, (1, 0): 3, (1, 1): 2}

    for k in range(2):

        @pl.when(core == k)
        def _():
            inputs, cotangent = (mine, received) if k == 0 else (received, mine)
            for g, y, f in itertools.product(range(2), range(4), range(2)):
                block = g * 4 + y if k == 0 else y * 2 + g
                z = position[g, f]
                rows, cols = slice(block * t, (block + 1) * t), slice(f * half, (f + 1) * half)
                x_ref[rows, cols] = inputs[z][y * t : (y + 1) * t]
                c_ref[rows, cols] = cotangent[y][z * t : (z + 1) * t]


def assemble(core, mine, received):
    rows, half = mine[3].shape
    shape = jax.ShapeDtypeStruct((2 * rows, 2 * half), BF16)
    return pl.pallas_call(
        assemble_body,
        out_shape=(shape,) * 2,
        in_specs=[SMEM] + [VMEM] * 8,
        out_specs=(VMEM,) * 2,
        compiler_params=pltpu.CompilerParams(vmem_limit_bytes=4 * 1024 * 1024),
        cost_estimate=pl.CostEstimate(flops=4_000_000, bytes_accessed=15_000_000, transcendentals=0),
        name="assemble",
    )(core.reshape(1), *mine, *received)


def per_device(inputs, cotangent, gate_weight, up_weight, down_weight):
    t, half = inputs.shape
    side, core = lax.axis_index("mp"), lax.axis_index(CORE)
    cat = jnp.concatenate
    hold = lax.optimization_barrier

    keep = jnp.where(core == 0, inputs, cotangent)
    give = jnp.where(core == 0, cotangent, inputs)
    first = cat([keep, shift(give, CORE, 1)])
    first, on_left = hold((first, side == 0))
    f, b = fetch(first, "y+", "P"), fetch(first, "y-", "Q")
    far = fetch(first, "y2", "PQ")
    g_own = hold(cat([v[:t] for v in (first, f, b, far)]))
    g_other = hold(cat([v[t:] for v in (first, f, b, far)]))
    a_own = fetch(g_own, "P", "y+")
    b_other = fetch(g_other, "Q", "y-")
    a_other = fetch(g_other, "P", "y+")
    b_own = fetch(g_own, "Q", "y-")
    n = 4 * t
    mine = (g_own, a_own, b_own, fetch(a_own, "Q", "y+"))
    received = (
        shift(g_other, CORE, 1),
        shift(a_other, CORE, 1),
        shift(b_other, CORE, 1),
        fetch(b_other, "P", "y-", cross=True),
    )

    own_w = prepare(side, gate_weight, up_weight, down_weight)
    wf, wb = shift(own_w, X, 1), shift(own_w, X, -1)
    wff = cat([shift(wf[:128], X, 1), shift(wb[128:], X, -1)])
    pieces = []
    for w in (own_w, wf, wb, wff):
        pieces += [w, shift(w, CORE, 1)]
    wgu = hold(cat([w[:ROWS] for w in pieces] + [w[ROWS : 2 * ROWS] for w in pieces]))
    wd = hold(cat([w[2 * ROWS :] for w in pieces]))
    ff = wd.shape[0]

    x, c = assemble(core, mine, received)
    x0, x1, c0, c1 = x[:n], x[n:], c[:n], c[n:]

    def hidden_grads(x, c):
        gate = rdot(wgu[:ff], x)
        up = rdot(wgu[ff:], x)
        dhidden = rdot(wd, c)
        sig = jax.nn.sigmoid(gate)
        act = gate * sig
        dup = (dhidden * act).astype(BF16)
        dgate = (dhidden * up * sig * (1.0 + gate * (1.0 - sig))).astype(BF16)
        return hold((dgate, dup))

    def input_partials(dgate, dup, order):
        gi = hold(
            lax.dot_general(
                cat([dgate, dup]), wgu, (((0,), (0,)), ((), ())), preferred_element_type=F32
            ).astype(BF16)
        )
        on_0 = (gi[:, :half], gi[:, half:])
        on_1 = []
        for k in order:
            v = gi[2 * k * t : 2 * (k + 1) * t]
            on_1.append(cat([v[:t, :half], v[:t, half:], v[t:, half:], v[t:, :half]]))
        return hold(tuple(jnp.where(core == 0, u, v) for u, v in zip(on_0, on_1)))

    dg1, du1 = hidden_grads(x1, c1)
    far_part, back_part = input_partials(dg1, du1, (1, 0))
    got_far = fetch(far_part, "PQ", "y2")
    got_back = fetch(back_part, "Q", "y+")
    x0, c0, far_part, back_part = hold((x0, c0, far_part, back_part))
    dg0, du0 = hidden_grads(x0, c0)
    own_part, fwd_part = input_partials(dg0, du0, (0, 1))
    got_fwd = fetch(fwd_part, "P", "y-")
    dg0, dg1, own_part, fwd_part = hold((dg0, dg1, own_part, fwd_part))

    gg = hold(jnp.dot(cat([dg0, dg1], axis=1), x, preferred_element_type=F32).astype(BF16))
    r = ROWS
    own = cat([gg[2 * k * r : (2 * k + 1) * r] for k in range(4)])
    theirs = cat([gg[(2 * k + 1) * r : (2 * k + 2) * r] for k in range(4)])
    theirs = shift(theirs, CORE, 1)
    cg = hold(total(own, theirs))
    gw = total(
        cg[:r],
        shift(cg[r : 2 * r], X, -1),
        shift(cg[2 * r : 3 * r], X, 1),
        shift(cg[3 * r :], X, 2),
    )

    s = total(own_part, got_fwd, got_back, got_far)
    s = hold(tuple(s[k * t : (k + 1) * t] for k in range(4)))
    input_grad = total(
        s[0], fetch(s[1], "y-", "P"), fetch(s[2], "y+", "Q"), fetch(s[3], "y2", "PQ")
    )

    gw = gw[: gate_weight.shape[0]]
    gate_grad = jnp.where(on_left, gw, cat([gw[:, half:], gw[:, :half]], axis=1))
    return input_grad, gate_grad


def solution(mesh):
    torus = Mesh(
        mesh.devices.reshape(2, 4, 4, 2, mesh.shape["mp"]), ("dp_0", "dp_1", "dp_2", "dp_3", "mp")
    )

    return jax.shard_map(
        per_device,
        mesh=torus,
        in_specs=(P(DP, "mp"), P(DP, "mp"), P(MP_DP, None), P(MP_DP, None), P(MP_DP, None)),
        out_specs=(P(DP, "mp"), P(MP_DP, None)),
        check_vma=False,
    )
```

```python
import itertools

import jax
import jax.numpy as jnp
from jax import lax
from jax.experimental import pallas as pl
from jax.experimental.pallas import tpu as pltpu
from jax.sharding import Mesh
from jax.sharding import PartitionSpec as P

DP = ("dp_0", "dp_1", "dp_2", "dp_3")
MP_DP = ("mp", "dp_0", "dp_1", "dp_2", "dp_3")
X, CORE = "dp_1", "dp_3"
PLANE = ("dp_0", "dp_2", "dp_3", "mp")
SIZES = (2, 4, 2, 2)


F32, BF16 = jnp.float32, jnp.bfloat16
ROWS = 80
VMEM = pl.BlockSpec(memory_space=pltpu.VMEM)
SMEM = pl.BlockSpec(memory_space=pltpu.SMEM)

MOVES = {
    "y+": lambda z, y: (z, (y + 1) % 4),
    "y-": lambda z, y: (z, (y - 1) % 4),
    "y2": lambda z, y: (z, (y + 2) % 4),
    "P": lambda z, y: (z ^ 1, y),
    "Q": lambda z, y: (3 - z, y),
    "PQ": lambda z, y: (z ^ 2, y),
}


def fetch(x, on_core_0, on_core_1, cross=False):
    pairs = []

    def index(zh, y, core, zl):
        return ((zh * SIZES[1] + y) * SIZES[2] + core) * SIZES[3] + zl

    for zh, y, core, zl in itertools.product(*(range(n) for n in SIZES)):
        sender = 1 - core if cross else core
        z_from, y_from = MOVES[on_core_1 if sender else on_core_0](zh * 2 + zl, y)
        pairs.append((index(z_from // 2, y_from, sender, z_from % 2), index(zh, y, core, zl)))
    return lax.ppermute(x, PLANE, pairs)


def shift(x, axis, by):
    n = lax.axis_size(axis)
    return lax.ppermute(x, axis, [(i, (i - by) % n) for i in range(n)])


def rdot(left, right):
    return lax.dot_general(left, right, (((1,), (1,)), ((), ())), preferred_element_type=F32)


def total(*parts):
    out = parts[0].astype(F32)
    for p in parts[1:]:
        out = out + p.astype(F32)
    return out.astype(BF16)


def prepare_body(side_ref, g_ref, u_ref, d_ref, out_ref):
    n, full = g_ref.shape
    half = full // 2
    side = side_ref[0]
    out_ref[...] = jnp.zeros_like(out_ref)
    for s in range(2):

        @pl.when(side == s)
        def _():
            for k, ref in enumerate((g_ref, u_ref, d_ref)):
                for f in range(2):
                    src = (f + s) % 2
                    out_ref[k * ROWS : k * ROWS + n, f * half : (f + 1) * half] = ref[
                        :, src * half : (src + 1) * half
                    ]


def prepare(side, gate_weight, up_weight, down_weight):
    full = gate_weight.shape[1]
    return pl.pallas_call(
        prepare_body,
        out_shape=jax.ShapeDtypeStruct((3 * ROWS, full), BF16),
        in_specs=[SMEM, VMEM, VMEM, VMEM],
        out_specs=VMEM,
        compiler_params=pltpu.CompilerParams(vmem_limit_bytes=8 * 1024 * 1024),
        cost_estimate=pl.CostEstimate(flops=2_000_000, bytes_accessed=1_700_000, transcendentals=0),
        name="prepare",
    )(side.reshape(1), gate_weight, up_weight, down_weight)


def assemble_body(core_ref, m0, m1, m2, m3, r0, r1, r2, r3, x_ref, c_ref):
    mine, received = (m0, m1, m2, m3), (r0, r1, r2, r3)
    half = m0.shape[1]
    t = m3.shape[0] // 4
    core = core_ref[0]
    position = {(0, 0): 0, (0, 1): 1, (1, 0): 3, (1, 1): 2}

    for k in range(2):

        @pl.when(core == k)
        def _():
            inputs, cotangent = (mine, received) if k == 0 else (received, mine)
            for g, y, f in itertools.product(range(2), range(4), range(2)):
                block = g * 4 + y if k == 0 else y * 2 + g
                z = position[g, f]
                rows, cols = slice(block * t, (block + 1) * t), slice(f * half, (f + 1) * half)
                x_ref[rows, cols] = inputs[z][y * t : (y + 1) * t]
                c_ref[rows, cols] = cotangent[y][z * t : (z + 1) * t]


def assemble(core, mine, received):
    rows, half = mine[3].shape
    shape = jax.ShapeDtypeStruct((2 * rows, 2 * half), BF16)
    return pl.pallas_call(
        assemble_body,
        out_shape=(shape,) * 2,
        in_specs=[SMEM] + [VMEM] * 8,
        out_specs=(VMEM,) * 2,
        compiler_params=pltpu.CompilerParams(vmem_limit_bytes=4 * 1024 * 1024),
        cost_estimate=pl.CostEstimate(flops=4_000_000, bytes_accessed=15_000_000, transcendentals=0),
        name="assemble",
    )(core.reshape(1), *mine, *received)


def per_device(inputs, cotangent, gate_weight, up_weight, down_weight):
    t, half = inputs.shape
    side, core = lax.axis_index("mp"), lax.axis_index(CORE)
    cat = jnp.concatenate
    hold = lax.optimization_barrier

    keep = jnp.where(core == 0, inputs, cotangent)
    give = jnp.where(core == 0, cotangent, inputs)
    first = cat([keep, shift(give, CORE, 1)])
    first, on_left = hold((first, side == 0))
    f, b = fetch(first, "y+", "P"), fetch(first, "y-", "Q")
    far = fetch(first, "y2", "PQ")
    g_own = hold(cat([v[:t] for v in (first, f, b, far)]))
    g_other = hold(cat([v[t:] for v in (first, f, b, far)]))
    a_own = fetch(g_own, "P", "y+")
    b_other = fetch(g_other, "Q", "y-")
    a_other = fetch(g_other, "P", "y+")
    b_own = fetch(g_own, "Q", "y-")
    n = 4 * t
    mine = (g_own, a_own, b_own, fetch(a_own, "Q", "y+"))
    received = (
        shift(g_other, CORE, 1),
        shift(a_other, CORE, 1),
        shift(b_other, CORE, 1),
        fetch(b_other, "P", "y-", cross=True),
    )

    own_w = prepare(side, gate_weight, up_weight, down_weight)
    wf, wb = shift(own_w, X, 1), shift(own_w, X, -1)
    wff = cat([shift(wf[:128], X, 1), shift(wb[128:], X, -1)])
    pieces = []
    for w in (own_w, wf, wb, wff):
        pieces += [w, shift(w, CORE, 1)]
    wgu = hold(cat([w[:ROWS] for w in pieces] + [w[ROWS : 2 * ROWS] for w in pieces]))
    wd = hold(cat([w[2 * ROWS :] for w in pieces]))
    ff = wd.shape[0]

    x, c = assemble(core, mine, received)
    x0, x1, c0, c1 = x[:n], x[n:], c[:n], c[n:]

    def hidden_grads(x, c):
        gate = rdot(wgu[:ff], x)
        up = rdot(wgu[ff:], x)
        dhidden = rdot(wd, c)
        sig = jax.nn.sigmoid(gate)
        act = gate * sig
        dup = (dhidden * act).astype(BF16)
        dgate = (dhidden * up * sig * (1.0 + gate * (1.0 - sig))).astype(BF16)
        return hold((dgate, dup))

    def input_partials(dgate, dup, order):
        gi = hold(
            lax.dot_general(
                cat([dgate, dup]), wgu, (((0,), (0,)), ((), ())), preferred_element_type=F32
            ).astype(BF16)
        )
        on_0 = (gi[:, :half], gi[:, half:])
        on_1 = []
        for k in order:
            v = gi[2 * k * t : 2 * (k + 1) * t]
            on_1.append(cat([v[:t, :half], v[:t, half:], v[t:, half:], v[t:, :half]]))
        return hold(tuple(jnp.where(core == 0, u, v) for u, v in zip(on_0, on_1)))

    dg1, du1 = hidden_grads(x1, c1)
    far_part, back_part = input_partials(dg1, du1, (1, 0))
    got_far = fetch(far_part, "PQ", "y2")
    got_back = fetch(back_part, "Q", "y+")
    x0, c0, far_part, back_part = hold((x0, c0, far_part, back_part))
    dg0, du0 = hidden_grads(x0, c0)
    r = ROWS
    dgate = cat([dg0, dg1], axis=1)
    dg_own = cat([dgate[2 * k * r : (2 * k + 1) * r] for k in range(4)])
    dg_theirs = cat([dgate[(2 * k + 1) * r : (2 * k + 2) * r] for k in range(4)])
    dg_own, dg_theirs = hold((dg_own, dg_theirs))
    theirs = hold(jnp.dot(dg_theirs, x, preferred_element_type=F32).astype(BF16))
    theirs = shift(theirs, CORE, 1)
    own_part, fwd_part = input_partials(dg0, du0, (0, 1))
    got_fwd = fetch(fwd_part, "P", "y-")
    own = hold(jnp.dot(dg_own, x, preferred_element_type=F32).astype(BF16))
    cg = hold(total(own, theirs))
    r = ROWS
    gw = total(
        cg[:r],
        shift(cg[r : 2 * r], X, -1),
        shift(cg[2 * r : 3 * r], X, 1),
        shift(cg[3 * r :], X, 2),
    )

    s = total(own_part, got_fwd, got_back, got_far)
    s = hold(tuple(s[k * t : (k + 1) * t] for k in range(4)))
    input_grad = total(
        s[0], fetch(s[1], "y-", "P"), fetch(s[2], "y+", "Q"), fetch(s[3], "y2", "PQ")
    )

    gw = gw[: gate_weight.shape[0]]
    gate_grad = jnp.where(on_left, gw, cat([gw[:, half:], gw[:, :half]], axis=1))
    return input_grad, gate_grad


def solution(mesh):
    torus = Mesh(
        mesh.devices.reshape(2, 4, 4, 2, mesh.shape["mp"]), ("dp_0", "dp_1", "dp_2", "dp_3", "mp")
    )

    return jax.shard_map(
        per_device,
        mesh=torus,
        in_specs=(P(DP, "mp"), P(DP, "mp"), P(MP_DP, None), P(MP_DP, None), P(MP_DP, None)),
        out_specs=(P(DP, "mp"), P(MP_DP, None)),
        check_vma=False,
    )
```

```python
import itertools

import jax
import jax.numpy as jnp
from jax import lax
from jax.experimental import pallas as pl
from jax.experimental.pallas import tpu as pltpu
from jax.sharding import Mesh
from jax.sharding import PartitionSpec as P

DP = ("dp_0", "dp_1", "dp_2", "dp_3")
MP_DP = ("mp", "dp_0", "dp_1", "dp_2", "dp_3")
X, CORE = "dp_1", "dp_3"
PLANE = ("dp_0", "dp_2", "dp_3", "mp")
SIZES = (2, 4, 2, 2)


F32, BF16 = jnp.float32, jnp.bfloat16
ROWS = 80
VMEM = pl.BlockSpec(memory_space=pltpu.VMEM)
SMEM = pl.BlockSpec(memory_space=pltpu.SMEM)

MOVES = {
    "y+": lambda z, y: (z, (y + 1) % 4),
    "y-": lambda z, y: (z, (y - 1) % 4),
    "y2": lambda z, y: (z, (y + 2) % 4),
    "P": lambda z, y: (z ^ 1, y),
    "Q": lambda z, y: (3 - z, y),
    "PQ": lambda z, y: (z ^ 2, y),
}


def fetch(x, on_core_0, on_core_1, cross=False):
    pairs = []

    def index(zh, y, core, zl):
        return ((zh * SIZES[1] + y) * SIZES[2] + core) * SIZES[3] + zl

    for zh, y, core, zl in itertools.product(*(range(n) for n in SIZES)):
        sender = 1 - core if cross else core
        z_from, y_from = MOVES[on_core_1 if sender else on_core_0](zh * 2 + zl, y)
        pairs.append((index(z_from // 2, y_from, sender, z_from % 2), index(zh, y, core, zl)))
    return lax.ppermute(x, PLANE, pairs)


def shift(x, axis, by):
    n = lax.axis_size(axis)
    return lax.ppermute(x, axis, [(i, (i - by) % n) for i in range(n)])


def rdot(left, right):
    return lax.dot_general(left, right, (((1,), (1,)), ((), ())), preferred_element_type=F32)


def total(*parts):
    out = parts[0].astype(F32)
    for p in parts[1:]:
        out = out + p.astype(F32)
    return out.astype(BF16)


def prepare_body(side_ref, g_ref, u_ref, d_ref, out_ref):
    n, full = g_ref.shape
    half = full // 2
    side = side_ref[0]
    out_ref[...] = jnp.zeros_like(out_ref)
    for s in range(2):

        @pl.when(side == s)
        def _():
            for k, ref in enumerate((g_ref, u_ref, d_ref)):
                for f in range(2):
                    src = (f + s) % 2
                    out_ref[k * ROWS : k * ROWS + n, f * half : (f + 1) * half] = ref[
                        :, src * half : (src + 1) * half
                    ]


def prepare(side, gate_weight, up_weight, down_weight):
    full = gate_weight.shape[1]
    return pl.pallas_call(
        prepare_body,
        out_shape=jax.ShapeDtypeStruct((3 * ROWS, full), BF16),
        in_specs=[SMEM, VMEM, VMEM, VMEM],
        out_specs=VMEM,
        compiler_params=pltpu.CompilerParams(vmem_limit_bytes=8 * 1024 * 1024),
        cost_estimate=pl.CostEstimate(flops=2_000_000, bytes_accessed=1_700_000, transcendentals=0),
        name="prepare",
    )(side.reshape(1), gate_weight, up_weight, down_weight)


def assemble_body(core_ref, m0, m1, m2, m3, r0, r1, r2, r3, x_ref, c_ref):
    mine, received = (m0, m1, m2, m3), (r0, r1, r2, r3)
    half = m0.shape[1]
    t = m3.shape[0] // 4
    core = core_ref[0]
    position = {(0, 0): 0, (0, 1): 1, (1, 0): 3, (1, 1): 2}

    for k in range(2):

        @pl.when(core == k)
        def _():
            inputs, cotangent = (mine, received) if k == 0 else (received, mine)
            for g, y, f in itertools.product(range(2), range(4), range(2)):
                block = g * 4 + y if k == 0 else y * 2 + g
                z = position[g, f]
                rows, cols = slice(block * t, (block + 1) * t), slice(f * half, (f + 1) * half)
                x_ref[rows, cols] = inputs[z][y * t : (y + 1) * t]
                c_ref[rows, cols] = cotangent[y][z * t : (z + 1) * t]


def assemble(core, mine, received):
    rows, half = mine[3].shape
    shape = jax.ShapeDtypeStruct((2 * rows, 2 * half), BF16)
    return pl.pallas_call(
        assemble_body,
        out_shape=(shape,) * 2,
        in_specs=[SMEM] + [VMEM] * 8,
        out_specs=(VMEM,) * 2,
        compiler_params=pltpu.CompilerParams(vmem_limit_bytes=4 * 1024 * 1024),
        cost_estimate=pl.CostEstimate(flops=4_000_000, bytes_accessed=15_000_000, transcendentals=0),
        name="assemble",
    )(core.reshape(1), *mine, *received)


def per_device(inputs, cotangent, gate_weight, up_weight, down_weight):
    t, half = inputs.shape
    side, core = lax.axis_index("mp"), lax.axis_index(CORE)
    cat = jnp.concatenate
    hold = lax.optimization_barrier

    keep = jnp.where(core == 0, inputs, cotangent)
    give = jnp.where(core == 0, cotangent, inputs)
    first = cat([keep, shift(give, CORE, 1)])
    first, on_left = hold((first, side == 0))
    f, b = fetch(first, "y+", "P"), fetch(first, "y-", "Q")
    far = fetch(first, "y2", "PQ")
    g_own = hold(cat([v[:t] for v in (first, f, b, far)]))
    g_other = hold(cat([v[t:] for v in (first, f, b, far)]))
    a_own = fetch(g_own, "P", "y+")
    b_other = fetch(g_other, "Q", "y-")
    a_other = fetch(g_other, "P", "y+")
    b_own = fetch(g_own, "Q", "y-")
    n = 4 * t
    mine = (g_own, a_own, b_own, fetch(a_own, "Q", "y+"))
    received = (
        shift(g_other, CORE, 1),
        shift(a_other, CORE, 1),
        shift(b_other, CORE, 1),
        fetch(b_other, "P", "y-", cross=True),
    )

    own_w = prepare(side, gate_weight, up_weight, down_weight)
    wf, wb = shift(own_w, X, 1), shift(own_w, X, -1)
    pieces = []
    for w in (own_w, wf, wb):
        pieces += [w, shift(w, CORE, 1)]
    wff = shift(wf[:128], X, 1), shift(wb[128:], X, -1)
    *wff, pieces[3], pieces[5], pass_b = hold((*wff, pieces[3], pieces[5], received[2]))
    received = (*received[:2], pass_b, received[3])
    wff = cat(wff)
    pieces += [wff, shift(wff, CORE, 1)]
    wgu = hold(cat([w[:ROWS] for w in pieces] + [w[ROWS : 2 * ROWS] for w in pieces]))
    wd = hold(cat([w[2 * ROWS :] for w in pieces]))
    ff = wd.shape[0]

    x, c = assemble(core, mine, received)
    x0, x1, c0, c1 = x[:n], x[n:], c[:n], c[n:]

    def hidden_grads(x, c):
        gate = rdot(wgu[:ff], x)
        up = rdot(wgu[ff:], x)
        dhidden = rdot(wd, c)
        sig = jax.nn.sigmoid(gate)
        act = gate * sig
        dup = (dhidden * act).astype(BF16)
        dgate = (dhidden * up * sig * (1.0 + gate * (1.0 - sig))).astype(BF16)
        return hold((dgate, dup))

    def input_partials(dgate, dup, order):
        gi = hold(
            lax.dot_general(
                cat([dgate, dup]), wgu, (((0,), (0,)), ((), ())), preferred_element_type=F32
            ).astype(BF16)
        )
        on_0 = (gi[:, :half], gi[:, half:])
        on_1 = []
        for k in order:
            v = gi[2 * k * t : 2 * (k + 1) * t]
            on_1.append(cat([v[:t, :half], v[:t, half:], v[t:, half:], v[t:, :half]]))
        return hold(tuple(jnp.where(core == 0, u, v) for u, v in zip(on_0, on_1)))

    dg1, du1 = hidden_grads(x1, c1)
    far_part, back_part = input_partials(dg1, du1, (1, 0))
    got_far = fetch(far_part, "PQ", "y2")
    got_back = fetch(back_part, "Q", "y+")
    x0, c0, far_part, back_part = hold((x0, c0, far_part, back_part))
    dg0, du0 = hidden_grads(x0, c0)
    r = ROWS
    dgate = cat([dg0, dg1], axis=1)
    dg_own = cat([dgate[2 * k * r : (2 * k + 1) * r] for k in range(4)])
    dg_theirs = cat([dgate[(2 * k + 1) * r : (2 * k + 2) * r] for k in range(4)])
    dg_own, dg_theirs = hold((dg_own, dg_theirs))
    theirs = hold(jnp.dot(dg_theirs, x, preferred_element_type=F32).astype(BF16))
    theirs = shift(theirs, CORE, 1)
    own_part, fwd_part = input_partials(dg0, du0, (0, 1))
    got_fwd = fetch(fwd_part, "P", "y-")
    own = hold(jnp.dot(dg_own, x, preferred_element_type=F32).astype(BF16))
    cg = hold(total(own, theirs))
    r = ROWS
    gw = total(
        cg[:r],
        shift(cg[r : 2 * r], X, -1),
        shift(cg[2 * r : 3 * r], X, 1),
        shift(cg[3 * r :], X, 2),
    )

    s = total(own_part, got_fwd, got_back, got_far)
    s = hold(tuple(s[k * t : (k + 1) * t] for k in range(4)))
    input_grad = total(
        s[0], fetch(s[1], "y-", "P"), fetch(s[2], "y+", "Q"), fetch(s[3], "y2", "PQ")
    )

    gw = gw[: gate_weight.shape[0]]
    gate_grad = jnp.where(on_left, gw, cat([gw[:, half:], gw[:, :half]], axis=1))
    return input_grad, gate_grad


def solution(mesh):
    torus = Mesh(
        mesh.devices.reshape(2, 4, 4, 2, mesh.shape["mp"]), ("dp_0", "dp_1", "dp_2", "dp_3", "mp")
    )

    return jax.shard_map(
        per_device,
        mesh=torus,
        in_specs=(P(DP, "mp"), P(DP, "mp"), P(MP_DP, None), P(MP_DP, None), P(MP_DP, None)),
        out_specs=(P(DP, "mp"), P(MP_DP, None)),
        check_vma=False,
    )
```
